512 devices in a mesh: dp: 16 (over y_lo, x), space: 32 (over z, y_hi, core).
Axes of the slice: x: 4, y: 8 (y_hi: 2, y_lo: 4; y = y_hi * 4 + y_lo), z: 8, core: 2. Of those that a mesh axis runs over, the one named last changes fastest.
Arguments:
- fields: bfloat16 [16, 100, 131072], P('dp', None, 'space'), may hold values from -6 to 6
- cell_index: int32 [1024, 128], P('space'), may hold values from 0 to 6143
- interp_weight: bfloat16 [1024, 16, 128], P('space'), may hold values from 0 to 2, as said below
- w_in: bfloat16 [100, 1024], replicated, may hold values from -0.625 to 0.625
- ln_gain: float32 [1024], replicated, may hold values from 0.5 to 1.5
- w_qkv: bfloat16 [1024, 3072], P('dp'), may hold values from -0.1875 to 0.1875
- w_out: bfloat16 [1024, 1024], P('dp'), may hold values from -3 to 3
Outputs:
- latent: bfloat16 [16, 16384, 1024], P('dp', 'space')
- update: bfloat16 [16, 16384, 1024], P('dp', 'space')
The draws below stay inside these ranges and needn't reach their ends.
Inputs may be any that keep to these rules, and one draw needn't show every extreme that they name: `interp_weight`: in each block the slots from some count on carry zero weight for all its 16 nodes; that count lies between 48 and 128. `cell_index`: indexes a shard's 4096 cells extended by 1024 cells of each neighbouring shard, lower neighbour first.
All inputs are finite; a program needn't handle non-finite values.
Results may differ from the reference program's by a relative error of at most 0.0068.
Values may be sent and summed in bfloat16 or wider, within the bound.
A program may use at most 128 MiB of HBM per device.

```python
import math
import jax
import jax.numpy as jnp
from jax import lax

D = 1024
HEADS = 16
CH = 100
NBLK = 16
SLOTS = 128
NODE_DEV = 512
CELL_DEV = 4096
HEAD_SIZE = 64
HALO_C = 1024
HALO_N = 256
BLK_DEV = 32
SAMPLES = 16
NODES = 16384
CELLS = 131072
BLOCKS = 1024
N_SPACE = 32


def draw_interp_weight(key, part):
    count_key, chosen_key, magnitude_key = jax.random.split(key, 3)
    full_shape = (BLOCKS, NBLK, SLOTS)
    live_count = jax.random.randint(count_key, (BLOCKS, 1, 1), 3 * SLOTS // 8, SLOTS + 1)
    slot_index = lax.broadcasted_iota(jnp.int32, full_shape, 2)
    chosen = jax.random.randint(chosen_key, full_shape, 0, 2)
    kept_mask = (slot_index < live_count) & (chosen == 0)
    magnitude = jax.random.uniform(magnitude_key, full_shape, jnp.float32, 0.0, 1.0)
    return jnp.where(kept_mask, magnitude, 0.0).astype(jnp.float32).astype(jnp.bfloat16)


def plant(array, rng, low, largest):
    spot = [jax.random.randint(jax.random.fold_in(rng, axis), (), 0, length) for axis, length in enumerate(array.shape)]
    longest = array.shape.index(max(array.shape))
    beside = spot[:longest] + [(spot[longest] + 1) % array.shape[longest]] + spot[longest + 1:]
    return array.at[tuple(spot)].set(low).at[tuple(beside)].set(largest)


def block_scale(stream_key, dims, shards, least, top_value):
    level, own = 1.0, jax.random.fold_in(stream_key, 6)
    for axis_at, shards_of in shards:
        heights = jnp.exp(jax.random.uniform(jax.random.fold_in(own, axis_at), (shards_of,), jnp.float32, least / len(shards), top_value / len(shards)))
        level = level * jnp.repeat(heights, dims[axis_at] // shards_of).reshape([-1 if axis == axis_at else 1 for axis in range(len(dims))])
    return level


def bell_draw(key, extent, width, bound, shards=(), kind=jnp.bfloat16):
    entries = width * jax.random.normal(key, extent, jnp.float32)
    if shards:
        entries = entries * block_scale(key, extent, shards, -0.22, 0.18)
    return jnp.clip(entries, -bound, bound).astype(kind)


def setup_inputs(seed: int = 0) -> dict:
    seeds = jax.random.split(jax.random.key(seed), 8)
    fields = bell_draw(seeds[0], (SAMPLES, CH, CELLS), 1.0, 6.0, ((0, 16), (2, 32)))
    cell_index = plant(jax.random.randint(seeds[1], (BLOCKS, SLOTS), 0, CELL_DEV + 2 * HALO_C), jax.random.fold_in(seeds[1], 1), 0, (CELL_DEV + 2 * HALO_C) - 1).astype(jnp.int32)
    interp_weight = draw_interp_weight(jax.random.fold_in(seeds[7], 71), 0)
    w_in = bell_draw(seeds[3], (CH, D), CH ** -0.5, 0.625)
    ln_gain = jnp.clip(1.0 + 0.1 * jax.random.normal(seeds[4], (D,), jnp.float32), 0.5, 1.5)
    w_qkv = bell_draw(seeds[5], (D, 3 * D), D ** -0.5, 0.1875, ((0, 16),))
    w_out = bell_draw(seeds[6], (D, D), (max(D // 256, 1)) ** -0.5, 3.0, ((0, 16),))
    return {"fields": fields, "cell_index": cell_index, "interp_weight": interp_weight, "w_in": w_in, "ln_gain": ln_gain, "w_qkv": w_qkv, "w_out": w_out}


def unit_heads(projected):
    head_rows = projected.reshape(projected.shape[0], HEADS, HEAD_SIZE)
    scale_rows = jnp.sqrt(lax.optimization_barrier(jnp.mean(head_rows * head_rows, axis=-1, keepdims=True)) + 1e-06)
    return (head_rows / scale_rows).astype(jnp.bfloat16)

def one_sample(grid_field, cell_index, interp_weight, w_in, ln_gain, w_qkv, w_out):
    owner_shard = jnp.arange(BLOCKS, dtype=jnp.int32) // BLK_DEV
    source = (owner_shard[:, None] * CELL_DEV - HALO_C + cell_index) % CELLS
    picked = jnp.take(grid_field, source.astype(jnp.int32), axis=1).astype(jnp.float32)
    encoded = jnp.einsum('cbs,bns->bnc', picked, interp_weight.astype(jnp.float32))
    encoded = encoded.reshape(NODES, CH).astype(jnp.bfloat16)
    embedded = jnp.dot(encoded, w_in, preferred_element_type=jnp.float32)
    average = lax.optimization_barrier(jnp.mean(embedded, axis=1, keepdims=True))
    centered = embedded - average
    spread = lax.optimization_barrier(jnp.mean(centered * centered, axis=1, keepdims=True))
    normed = (centered / jnp.sqrt(spread + 1e-05) * ln_gain).astype(jnp.bfloat16)
    projected = jnp.dot(normed, w_qkv, preferred_element_type=jnp.float32)
    queries = unit_heads(projected[:, :D])
    keys_all = unit_heads(projected[:, D:2 * D])
    values_all = projected[:, 2 * D:].reshape(NODES, HEADS, HEAD_SIZE).astype(jnp.bfloat16)
    wrapped_keys = jnp.concatenate([keys_all[NODES - HALO_N:], keys_all, keys_all[:HALO_N]], axis=0)
    wrapped_values = jnp.concatenate([values_all[NODES - HALO_N:], values_all, values_all[:HALO_N]], axis=0)

    def attend(shard_index):
        first_row = shard_index * NODE_DEV
        query_rows = lax.dynamic_slice_in_dim(queries, first_row, NODE_DEV, 0).astype(jnp.float32)
        key_rows = lax.dynamic_slice_in_dim(wrapped_keys, first_row, NODE_DEV + 2 * HALO_N, 0).astype(jnp.float32)
        value_rows = lax.dynamic_slice_in_dim(wrapped_values, first_row, NODE_DEV + 2 * HALO_N, 0).astype(jnp.float32)
        scores = jnp.einsum('qhd,khd->hqk', query_rows, key_rows) / math.sqrt(HEAD_SIZE)
        weights = jnp.exp(scores)
        probs = (weights / lax.optimization_barrier(jnp.sum(weights, axis=2, keepdims=True))).astype(jnp.bfloat16)
        mixed_rows = jnp.einsum('hqk,khd->qhd', probs.astype(jnp.float32), value_rows)
        return mixed_rows.astype(jnp.bfloat16).reshape(NODE_DEV, D)
    attended = lax.map(attend, jnp.arange(N_SPACE, dtype=jnp.int32)).reshape(NODES, D)
    update = jnp.dot(attended, w_out, preferred_element_type=jnp.float32).astype(jnp.bfloat16)
    return (embedded.astype(jnp.bfloat16), update)

def reference(fields, cell_index, interp_weight, w_in, ln_gain, w_qkv, w_out):

    def per_sample(grid_field):
        return one_sample(grid_field, cell_index, interp_weight, w_in, ln_gain, w_qkv, w_out)
    latent, update = lax.map(per_sample, fields)
    return (latent, update)
```

```python
import functools

import jax
import jax.numpy as jnp
from jax import lax
from jax.experimental import pallas as pl
from jax.experimental.pallas import tpu as pltpu
from jax.sharding import PartitionSpec as P

HEADS = 16
GROUP_HEADS = 4
F32, BF16 = jnp.float32, jnp.bfloat16
MESH = pl.DeviceIdType.MESH
OFFS = (0, -1, 1, 2)


def device_at(x, y, z, core):
    return lax.rem(y, 4) * 4 + x, z * 4 + (y // 4) * 2 + core


def kernel(
    index_hbm, field_hbm, weight_hbm, w_in_hbm, gain_hbm, w_qkv_hbm, w_out_hbm,
    att_out, w_out_full, enc_out,
    index_ref, field_ref, weight_ref, w_in_ref, gain_ref,
    low_ref, high_ref, cells_ref, picked_ref, enc_ref, w_in_full, normed_ref, qkv_ref, out_ref,
    q_ref, k_ref, v_ref, att_ref, stage_ref,
    load_sem, local_sem, leave_sem, field_send, field_recv, enc_send, enc_recv,
    nm_send, nm_recv, st_send, st_recv, sw_send, sw_recv, a_send, a_recv, ready_sem,
):
    d, s = lax.axis_index("dp"), lax.axis_index("space")
    x, y_low = lax.rem(d, 4), d // 4
    core, y_high, z = lax.rem(s, 2), lax.rem(s // 2, 2), s // 4
    y = y_high * 4 + y_low
    up, down = lax.rem(s + 1, 32), lax.rem(s + 31, 32)
    other = 1 - core
    partner = (d, s + 1 - 2 * core)
    far = (d, down + core * (up - down))
    wraps = (z == 0) & (y_high == 0) & (core == 0)
    wrapped = (z == 7) & (y_high == 1) & (core == 1)
    follows = ((core == 0) & jnp.logical_not(wraps)) | wrapped
    follow = follows.astype(jnp.int32)

    x_up, x_down = device_at(lax.rem(x + 1, 4), y, z, core), device_at(lax.rem(x + 3, 4), y, z, core)
    y_up, y_down = device_at(x, lax.rem(y + 1, 8), z, core), device_at(x, lax.rem(y + 7, 8), z, core)

    def either(first, second):
        return tuple(a + core * (b - a) for a, b in zip(first, second))

    p1, m1 = either(x_up, y_up), either(x_down, y_down)
    p2, m2 = either(y_up, x_up), either(y_down, x_down)
    stride1, stride2 = 1 + 3 * core, 4 - 3 * core
    place1, place2 = x + core * (y_low - x), y_low + core * (x - y_low)

    barrier = pltpu.get_barrier_semaphore()
    for peer in (p1, m1, p2, m2, partner):
        pl.semaphore_signal(barrier, inc=1, device_id=peer, device_id_type=MESH)

    @pl.when(jnp.logical_not(follows))
    def _():
        pl.semaphore_signal(barrier, inc=1, device_id=far, device_id_type=MESH)

    channels, cell_count = field_ref.shape
    reach = low_ref.shape[1]
    rows = w_qkv_hbm.shape[0]
    width = w_out_hbm.shape[1]
    groups, _, gw3 = qkv_ref.shape
    gw = gw3 // 3
    head_size = gw // GROUP_HEADS
    nodes = att_ref.shape[1]
    margin = nodes // 2
    window = nodes + 2 * margin
    blocks, per_block, slots = weight_ref.shape

    loads = [
        pltpu.make_async_copy(src, dst, load_sem.at[i])
        for i, (src, dst) in enumerate((
            (field_hbm, field_ref), (index_hbm, index_ref), (weight_hbm, weight_ref),
            (w_in_hbm, w_in_ref), (gain_hbm, gain_ref)))]
    local = []
    for g in range(groups):
        for t in range(3):
            local.append(pltpu.make_async_copy(
                w_qkv_hbm.at[:, pl.ds(pl.multiple_of(t * width + core * (width // 2) + g * gw, gw), gw)],
                qkv_ref.at[g, pl.ds(pl.multiple_of(d * rows, rows), rows), pl.ds(t * gw, gw)],
                local_sem.at[len(local)]))
    half = rows // 2
    local.append(pltpu.make_async_copy(
        w_out_hbm.at[pl.ds(pl.multiple_of(core * half, half), half), :], out_ref.at[d, core],
        local_sem.at[len(local)]))
    for copy in local[:3] + loads[:1] + local[3:] + loads[1:]:
        copy.start()

    pl.semaphore_wait(barrier, 5 + follow)

    @pl.when(follows)
    def _():
        pl.semaphore_signal(ready_sem, inc=1, device_id=far, device_id_type=MESH)

    def remote(src, dst, send, recv, device):
        return pltpu.make_async_remote_copy(
            src_ref=src, dst_ref=dst, send_sem=send, recv_sem=recv,
            device_id=device, device_id_type=MESH)

    field_up = remote(field_hbm.at[:, pl.ds(cell_count - reach, reach)], low_ref,
                      field_send.at[0], field_recv.at[0], (d, up))
    field_down = remote(field_hbm.at[:, pl.ds(0, reach)], high_ref,
                        field_send.at[1], field_recv.at[1], (d, down))

    def to_far():
        @pl.when(core == 0)
        def _():
            field_down.start()

        @pl.when(core == 1)
        def _():
            field_up.start()

    def far_when(role):
        @pl.when(role & jnp.logical_not(follows))
        def _():
            pl.semaphore_wait(ready_sem, 1)
            to_far()

    @pl.when(core == 0)
    def _():
        field_up.start()

    @pl.when(core == 1)
    def _():
        field_down.start()

    @pl.when(follows)
    def _():
        to_far()

    def slot(i, j):
        return lax.rem(place1 + i + 4, 4) * stride1 + lax.rem(place2 + j + 4, 4) * stride2

    def piece(c, at, side=None):
        if c < groups:
            lo, size = (0, rows) if side is None else (side * half, half)
            return qkv_ref.at[c, pl.ds(pl.multiple_of(at * rows + lo, size), size), :]
        lo, size = (0, half) if side is None else (side * (half // 2), half // 2)
        return out_ref.at[at, core, pl.ds(lo, size), :]

    def hop(c, i, ref, device):
        return remote(ref, ref, a_send.at[c, i], a_recv.at[c, i], device)

    def spread(c, j):
        ref = piece(c, slot(OFFS[j], 0))
        hop(c, 4 + 4 * j, ref, p2).start()
        hop(c, 5 + 4 * j, ref, m2).start()

    def begin(c):
        for copy in local[3 * c:3 * c + 3] if c < groups else local[-1:]:
            copy.wait()
        own = piece(c, slot(0, 0))
        hop(c, 0, own, p1).start()
        hop(c, 1, own, m1).start()
        spread(c, 0)

    def first(c):
        before, after = slot(-1, 0), slot(1, 0)
        hop(c, 0, piece(c, before), p1).wait_recv()
        hop(c, 2, piece(c, before, 0), p1).start()
        spread(c, 1)
        hop(c, 1, piece(c, after), p1).wait_recv()
        hop(c, 3, piece(c, after, 1), m1).start()
        spread(c, 2)

    def second(c):
        at = slot(2, 0)
        hop(c, 2, piece(c, at, 0), p1).wait_recv()
        hop(c, 3, piece(c, at, 1), p1).wait_recv()
        spread(c, 3)

    def across(c, j):
        before, after = slot(OFFS[j], -1), slot(OFFS[j], 1)
        hop(c, 4 + 4 * j, piece(c, before), p2).wait_recv()
        hop(c, 6 + 4 * j, piece(c, before, 0), p2).start()
        hop(c, 5 + 4 * j, piece(c, after), p2).wait_recv()
        hop(c, 7 + 4 * j, piece(c, after, 1), m2).start()

    def last(c):
        for j in range(4):
            at = slot(OFFS[j], 2)
            hop(c, 6 + 4 * j, piece(c, at, 0), p2).wait_recv()
            hop(c, 7 + 4 * j, piece(c, at, 1), p2).wait_recv()

    def drain(c):
        for i in range(20):
            ref = piece(c, slot(0, 0), 0 if i % 4 >= 2 else None)
            hop(c, i, ref, p1).wait_send()

    begin(0)
    begin(1)
    far_when(jnp.logical_not(wraps))

    unit = (lax.broadcasted_iota(jnp.int32, (channels, 128), 0)
            == lax.broadcasted_iota(jnp.int32, (channels, 128), 1)).astype(BF16)

    def turn(source, start, target):
        cells_ref[pl.ds(target, 512), :] = lax.dot_general(
            source[:, pl.ds(start, 512)], unit, (((0,), (0,)), ((), ())),
            preferred_element_type=F32)

    for copy in loads:
        copy.wait()

    @pl.loop(0, cell_count // 512, unroll=2)
    def _(i):
        turn(field_ref, pl.multiple_of(i * 512, 512), pl.multiple_of(reach + i * 512, 512))

    pad = w_in_full.shape[0]
    w_in_full[pl.ds(pad - 32, 32), :] = jnp.zeros((32, width), BF16)
    w_in_full[pl.ds(0, channels), :] = w_in_ref[...]

    first(0)
    across(0, 0)
    first(1)
    begin(groups)
    far_when(wraps)

    field_up.wait_recv()
    field_down.wait_recv()

    @pl.loop(0, reach // 512)
    def _(i):
        turn(low_ref, pl.multiple_of(i * 512, 512), pl.multiple_of(i * 512, 512))
        turn(high_ref, pl.multiple_of(i * 512, 512),
             pl.multiple_of(reach + cell_count + i * 512, 512))

    def gather(begin_at, end_at):
        @pl.loop(begin_at, end_at)
        def _(b):
            base = pl.multiple_of(b * slots, slots)
            for j in range(slots):
                picked_ref[pl.ds(base + j, 1), :] = cells_ref[pl.ds(index_ref[b, j], 1), :]

    across(1, 0)
    second(0)
    gather(0, blocks // 2)
    across(0, 1)
    across(0, 2)
    second(1)
    first(groups)
    gather(blocks // 2, blocks)
    across(0, 3)
    across(1, 1)
    across(1, 2)

    per_step = 8

    @pl.loop(0, blocks // per_step)
    def _(i):
        for j in range(per_step):
            b = i * per_step + j
            rows_b = picked_ref[pl.ds(pl.multiple_of(b * slots, slots), slots), :].astype(BF16)
            enc_ref[pl.ds(pl.multiple_of(b * per_block, per_block), per_block), :] = jnp.dot(
                weight_ref[b], rows_b, preferred_element_type=F32).astype(BF16)

    enc_far = remote(enc_ref.at[pl.ds(pl.multiple_of(core * margin, margin), margin), :],
                     enc_ref.at[pl.ds(nodes, margin), :], enc_send.at[0], enc_recv.at[0], far)
    enc_far.start()
    enc_leave = pltpu.make_async_copy(enc_ref.at[pl.ds(0, nodes), :], enc_out, leave_sem.at[0])
    enc_leave.start()

    def embed(start, target):
        embedded = jnp.dot(enc_ref[pl.ds(start, 128), :], w_in_full[...], preferred_element_type=F32)
        average = jnp.mean(embedded, axis=1, keepdims=True)
        centered = embedded - average
        spread_of = jnp.mean(centered * centered, axis=1, keepdims=True)
        normed_ref[pl.ds(target, 128), :] = (
            centered * lax.rsqrt(spread_of + 1e-05) * gain_ref[...]).astype(BF16)

    own = pl.multiple_of(margin + core * nodes, margin)
    theirs = pl.multiple_of(margin + other * nodes, margin)
    edge = pl.multiple_of(core * (window + nodes - margin), margin)
    their_edge = pl.multiple_of(other * (window + nodes - margin), margin)

    def share(i, start):
        ref = normed_ref.at[pl.ds(start, margin), :]
        return remote(ref, ref, nm_send.at[i], nm_recv.at[i], partner)

    for h in range(2):
        @pl.loop(0, 2, unroll=2)
        def _(i):
            embed(pl.multiple_of(h * margin + i * 128, 128), pl.multiple_of(own + h * margin + i * 128, 128))
        share(h, own + h * margin).start()
        if h == 0:
            across(1, 3)
            second(groups)
        else:
            across(groups, 0)

    same_head = (lax.broadcasted_iota(jnp.int32, (gw, gw), 0) // head_size
                 == lax.broadcasted_iota(jnp.int32, (gw, gw), 1) // head_size).astype(BF16)
    contract_last = (((1,), (1,)), ((), ()))

    def unit_heads(block, scale):
        squares = block * block
        high = squares.astype(BF16)
        rest = (squares - high.astype(F32)).astype(BF16)
        total = (jnp.dot(high, same_head, preferred_element_type=F32)
                 + jnp.dot(rest, same_head, preferred_element_type=F32))
        return (block * lax.rsqrt(total * (1.0 / head_size) + 1e-06)).astype(BF16) * scale

    scale = jnp.asarray(head_size ** -0.5, BF16)
    one = jnp.asarray(1.0, BF16)

    def keys_of(g, start, size):
        span = pl.ds(start, size)
        part = jnp.dot(normed_ref[span, :], qkv_ref[g, :, pl.ds(gw, 2 * gw)], preferred_element_type=F32)
        k_ref[g, span, :] = unit_heads(part[:, :gw], one)
        v_ref[g, span, :] = part[:, gw:].astype(BF16)

    def queries_of(g, start, size):
        part = jnp.dot(normed_ref[pl.ds(start, size), :], qkv_ref[g, :, pl.ds(0, gw)],
                       preferred_element_type=F32)
        q_ref[g, pl.ds(pl.multiple_of(start - margin, margin), size), :] = unit_heads(part, scale)

    last(0)
    last(1)

    @pl.loop(0, groups)
    def _(g):
        keys_of(g, own, nodes)
        queries_of(g, own, nodes)

    across(groups, 1)
    across(groups, 2)
    across(groups, 3)
    enc_far.wait_recv()

    @pl.loop(0, 2, unroll=2)
    def _(i):
        embed(pl.multiple_of(nodes + i * 128, 128), pl.multiple_of(edge + i * 128, 128))

    share(2, edge).start()
    share(0, theirs).wait_recv()
    share(1, theirs).wait_recv()

    @pl.loop(0, groups)
    def _(g):
        keys_of(g, theirs, nodes)
        queries_of(g, theirs, nodes)
        keys_of(g, edge, margin)

    last(groups)
    swap = remote(out_ref.at[:, core], out_ref.at[:, core], sw_send.at[0], sw_recv.at[0], partner)
    swap.start()
    share(2, their_edge).wait_recv()

    @pl.loop(0, groups)
    def _(g):
        keys_of(g, their_edge, margin)

    def attend(g, side, store):
        base = pl.multiple_of(side * nodes, nodes)

        @pl.loop(0, nodes // 128, unroll=2)
        def _(i):
            queries = q_ref[g, pl.ds(pl.multiple_of(base + i * 128, 128), 128), :]
            head_of = lax.broadcasted_iota(jnp.int32, (128, gw), 1) // head_size
            stacked = jnp.concatenate(
                [jnp.where(head_of == h, queries, jnp.zeros_like(queries))
                 for h in range(GROUP_HEADS)], axis=0)
            scores = lax.dot_general(stacked, k_ref[g, pl.ds(base, window), :], contract_last,
                                     preferred_element_type=F32)
            weights = jnp.exp(scores)
            total = jnp.sum(weights, axis=1, keepdims=True)
            out = jnp.dot(weights.astype(BF16), v_ref[g, pl.ds(base, window), :],
                          preferred_element_type=F32)
            out = out * (1.0 / total)
            mixed = out[:128]
            for h in range(1, GROUP_HEADS):
                mixed = jnp.where(head_of == h, out[h * 128:(h + 1) * 128], mixed)
            store(pl.ds(pl.multiple_of(i * 128, 128), 128), mixed.astype(BF16))

    def leave(i, j):
        return pltpu.make_async_copy(
            att_ref.at[j], att_out.at[:, pl.ds(pl.multiple_of(j * gw, gw), gw)], leave_sem.at[2 + i])

    def give(g):
        return remote(stage_ref.at[g], att_ref.at[core * groups + g], st_send.at[g], st_recv.at[g], partner)

    w_out_leave = pltpu.make_async_copy(out_ref, w_out_full, leave_sem.at[1])

    for g in range(groups):
        def to_stage(span, value):
            stage_ref[g, span, :] = value

        def to_own(span, value):
            att_ref[core * groups + g, span, :] = value

        attend(g, other, to_stage)
        give(g).start()
        attend(g, core, to_own)
        leave(g, core * groups + g).start()
        if g == 0:
            swap.wait_recv()
            w_out_leave.start()

    for g in range(groups):
        give(g).wait_recv()
        leave(groups + g, other * groups + g).start()
    for g in range(groups):
        leave(g, core * groups + g).wait()
        leave(groups + g, other * groups + g).wait()
    w_out_leave.wait()
    enc_leave.wait()
    for copy in (field_up, field_down, enc_far, swap):
        copy.wait_send()
    for i in range(3):
        share(i, own).wait_send()
    for g in range(groups):
        give(g).wait_send()
    for c in range(groups + 1):
        drain(c)


def project(enc_ref, w_in_ref, att_ref, w_out_ref, latent_ref, update_ref):
    channels = w_in_ref.shape[0]
    latent_ref[...] = jnp.dot(enc_ref[:, :channels], w_in_ref[...],
                              preferred_element_type=F32).astype(BF16)
    update_ref[...] = jnp.dot(att_ref[...], w_out_ref[...],
                              preferred_element_type=F32).astype(BF16)


def shards(n, fields, cell_index, interp_weight, w_in, ln_gain, w_qkv, w_out):
    width = w_out.shape[1]
    blocks, per_block, slots = interp_weight.shape
    nodes = blocks * per_block
    channels, cells = fields.shape[1:]
    reach = cells // 4
    gw = width // HEADS * GROUP_HEADS
    groups = width // gw // 2
    half = w_out.shape[0] // 2
    hbm = pl.BlockSpec(memory_space=pl.ANY)
    dma = pltpu.SemaphoreType.DMA
    attended, w_out_full, encoded = pl.pallas_call(
        kernel,
        out_shape=[jax.ShapeDtypeStruct(shape, BF16)
                   for shape in ((nodes, width), (n, 2, half, width), (nodes, 128))],
        in_specs=[hbm] * 7,
        out_specs=[hbm, hbm, hbm],
        scratch_shapes=[
            pltpu.SMEM((blocks, slots), jnp.int32),
            pltpu.VMEM((channels, cells), BF16),
            pltpu.VMEM((blocks, per_block, slots), BF16),
            pltpu.VMEM((channels, width), BF16),
            pltpu.VMEM((1, width), F32),
            pltpu.VMEM((channels, reach), BF16),
            pltpu.VMEM((channels, reach), BF16),
            pltpu.VMEM((cells + 2 * reach, 128), F32),
            pltpu.VMEM((blocks * 128, 128), F32),
            pltpu.VMEM((nodes + nodes // 2, 128), BF16),
            pltpu.VMEM((128, width), BF16),
            pltpu.VMEM((3 * nodes, width), BF16),
            pltpu.VMEM((groups, width, 3 * gw), BF16),
            pltpu.VMEM((n, 2, half, width), BF16),
            pltpu.VMEM((groups, 2 * nodes, gw), BF16),
            pltpu.VMEM((groups, 3 * nodes, gw), BF16),
            pltpu.VMEM((groups, 3 * nodes, gw), BF16),
            pltpu.VMEM((2 * groups, nodes, gw), BF16),
            pltpu.VMEM((groups, nodes, gw), BF16),
            dma((5,)), dma((3 * groups + 1,)), dma((2 * groups + 2,)),
            dma((2,)), dma((2,)), dma((1,)), dma((1,)),
            dma((3,)), dma((3,)), dma((groups,)), dma((groups,)), dma((1,)), dma((1,)),
            dma((groups + 1, 20)), dma((groups + 1, 20)),
            pltpu.SemaphoreType.REGULAR,
        ],
        compiler_params=pltpu.CompilerParams(
            collective_id=0, has_side_effects=True, vmem_limit_bytes=60 * 2**20),
    )(cell_index, fields[0], interp_weight, w_in, ln_gain[None], w_qkv, w_out)
    w_out_full = w_out_full.reshape(width, width)
    step = nodes // 2

    def by_row(size):
        return pl.BlockSpec((step, size), lambda i: (i, 0))

    def whole(array):
        return pl.BlockSpec(array.shape, lambda i: (0, 0))

    latent, update = pl.pallas_call(
        project,
        grid=(nodes // step,),
        out_shape=[jax.ShapeDtypeStruct((nodes, width), BF16)] * 2,
        in_specs=[by_row(128), whole(w_in), by_row(width), whole(w_out_full)],
        out_specs=[by_row(width), by_row(width)],
    )(encoded, w_in, attended, w_out_full)
    return latent[None], update[None]


def solution(mesh):
    placed = (
        P("dp", None, "space"),
        P("space", None),
        P("space", None, None),
        P(),
        P(),
        P("dp", None),
        P("dp", None),
    )
    return jax.shard_map(
        functools.partial(shards, mesh.shape["dp"]),
        mesh=mesh,
        in_specs=placed,
        out_specs=(P("dp", "space", None), P("dp", "space", None)),
        check_vma=False,
    )
```

```python
import functools

import jax
import jax.numpy as jnp
from jax import lax
from jax.experimental import pallas as pl
from jax.experimental.pallas import tpu as pltpu
from jax.sharding import PartitionSpec as P

HEADS = 16
GROUP_HEADS = 4
F32, BF16 = jnp.float32, jnp.bfloat16
MESH = pl.DeviceIdType.MESH
OFFS = (0, -1, 1, 2)


def either(flag, first, second):
    return second if flag else first


def device_at(x, y, z, core):
    return lax.rem(y, 4) * 4 + x, z * 4 + (y // 4) * 2 + core


def kernel(
    index_hbm, field_hbm, weight_hbm, w_in_hbm, gain_hbm, w_qkv_hbm, w_out_hbm,
    att_out, out_ref, enc_out, w_in_out,
    index_ref, field_ref, weight_ref, w_in_ref, gain_ref,
    low_ref, high_ref, cells_ref, picked_ref, enc_ref, w_in_full, normed_ref, qkv_ref,
    q_ref, k_ref, v_ref, att_ref, stage_ref,
    load_sem, local_sem, leave_sem, field_send, field_recv, enc_send, enc_recv,
    nm_send, nm_recv, st_send, st_recv, sw_send, sw_recv, a_send, a_recv, ready_sem,
):
    d, s = lax.axis_index("dp"), lax.axis_index("space")
    x, y_low = lax.rem(d, 4), d // 4
    core, y_high, z = lax.rem(s, 2), lax.rem(s // 2, 2), s // 4
    y = y_high * 4 + y_low
    up, down = lax.rem(s + 1, 32), lax.rem(s + 31, 32)
    other = 1 - core
    partner = (d, s + 1 - 2 * core)
    far = (d, down + core * (up - down))
    wraps, wrapped = s == 0, s == 31

    along_x = [device_at(lax.rem(x + i, 4), y, z, core) for i in (1, 3, 2, 2)]
    along_y = [device_at(x, lax.rem(y + i, 8), z, core) for i in (1, 7, 2, 6)]
    near = along_x[:3] + along_y + [partner]

    barrier = pltpu.get_barrier_semaphore()
    for peer in near:
        pl.semaphore_signal(barrier, inc=1, device_id=peer, device_id_type=MESH)

    @pl.when(jnp.logical_not(wrapped))
    def _():
        pl.semaphore_signal(barrier, inc=1, device_id=far, device_id_type=MESH)

    channels, cell_count = field_ref.shape
    reach = low_ref.shape[1]
    rows = w_qkv_hbm.shape[0]
    width = w_out_hbm.shape[1]
    groups, _, gw3 = qkv_ref.shape
    gw = gw3 // 3
    head_size = gw // GROUP_HEADS
    nodes = att_ref.shape[1]
    margin = nodes // 2
    window = nodes + 2 * margin
    blocks, per_block, slots = weight_ref.shape

    loads = [
        pltpu.make_async_copy(src, dst, load_sem.at[i])
        for i, (src, dst) in enumerate((
            (field_hbm, field_ref), (index_hbm, index_ref), (weight_hbm, weight_ref),
            (w_in_hbm, w_in_ref), (gain_hbm, gain_ref)))]
    local = []
    for g in range(groups):
        for t in range(3):
            local.append(pltpu.make_async_copy(
                w_qkv_hbm.at[:, pl.ds(pl.multiple_of(t * width + core * (width // 2) + g * gw, gw), gw)],
                qkv_ref.at[g, pl.ds(pl.multiple_of(d * rows, rows), rows), pl.ds(t * gw, gw)],
                local_sem.at[len(local)]))
    half = rows // 2
    local.append(pltpu.make_async_copy(
        w_out_hbm.at[pl.ds(pl.multiple_of(core * half, half), half), :], out_ref.at[d, core],
        local_sem.at[len(local)]))
    for copy in local[:3] + loads[:1] + local[3:] + loads[1:]:
        copy.start()

    pl.semaphore_wait(barrier, len(near) + 1 - wraps.astype(jnp.int32))

    @pl.when(wrapped)
    def _():
        pl.semaphore_signal(ready_sem, inc=1, device_id=far, device_id_type=MESH)

    def remote(src, dst, send, recv, device):
        return pltpu.make_async_remote_copy(
            src_ref=src, dst_ref=dst, send_sem=send, recv_sem=recv,
            device_id=device, device_id_type=MESH)

    field_up = remote(field_hbm.at[:, pl.ds(cell_count - reach, reach)], low_ref,
                      field_send.at[0], field_recv.at[0], (d, up))
    field_down = remote(field_hbm.at[:, pl.ds(0, reach)], high_ref,
                        field_send.at[1], field_recv.at[1], (d, down))

    def to_far():
        @pl.when(core == 0)
        def _():
            field_down.start()

        @pl.when(core == 1)
        def _():
            field_up.start()

    @pl.when(core == 0)
    def _():
        field_up.start()

    @pl.when(core == 1)
    def _():
        field_down.start()

    turns = (1, 1, 0)

    def slot(c, i, j):
        place1, place2 = x + turns[c] * (y_low - x), y_low + turns[c] * (x - y_low)
        return (lax.rem(place1 + i + 4, 4) * (1 + 3 * turns[c])
                + lax.rem(place2 + j + 4, 4) * (4 - 3 * turns[c]))

    def piece(c, at, side=None):
        if c < groups:
            lo, size = (0, rows) if side is None else (side * half, half)
            return qkv_ref.at[c, pl.ds(pl.multiple_of(at * rows + lo, size), size), :]
        lo, size = (0, half) if side is None else (side * (half // 2), half // 2)
        return out_ref.at[at, core, pl.ds(lo, size), :]

    sides = (None, None, 0, 1)

    def hop(c, i, at, device):
        ref = piece(c, at, sides[i % 4])
        return remote(ref, ref, a_send.at[c, i], a_recv.at[c, i], device)

    def begin(c):
        for copy in local[3 * c:3 * c + 3] if c < groups else local[-1:]:
            copy.wait()
        for i in range(4):
            hop(c, i, slot(c, 0, 0), either(turns[c], along_x[i], along_y[i])).start()

    def spread(c, j):
        for i in range(2):
            hop(c, 4 + 4 * j + i, slot(c, OFFS[j], 0), either(turns[c], along_y[i], along_x[i])).start()

    def onward(c):
        hop(c, 0, slot(c, -1, 0), partner).wait_recv()
        spread(c, 1)
        hop(c, 1, slot(c, 1, 0), partner).wait_recv()
        spread(c, 2)
        hop(c, 2, slot(c, 2, 0), partner).wait_recv()
        hop(c, 3, slot(c, 2, 0), partner).wait_recv()
        spread(c, 3)

    def across(c, *js):
        for j in js:
            for i in range(2):
                at = slot(c, OFFS[j], 2 * i - 1)
                hop(c, 4 + 4 * j + i, at, partner).wait_recv()
                hop(c, 6 + 4 * j + i, at, either(turns[c], along_y[i], along_x[i])).start()

    def last(c):
        for j in range(4):
            for i in range(2):
                hop(c, 6 + 4 * j + i, slot(c, OFFS[j], 2), partner).wait_recv()

    def drain(c):
        for i in range(20):
            hop(c, i, slot(c, 0, 0), partner).wait_send()

    @pl.when(wrapped)
    def _():
        to_far()

    begin(0)

    @pl.when(jnp.logical_not(wraps | wrapped))
    def _():
        to_far()

    spread(0, 0)

    unit = (lax.broadcasted_iota(jnp.int32, (channels, 128), 0)
            == lax.broadcasted_iota(jnp.int32, (channels, 128), 1)).astype(BF16)

    def turn(source, start, target):
        cells_ref[pl.ds(target, 512), :] = lax.dot_general(
            source[:, pl.ds(start, 512)], unit, (((0,), (0,)), ((), ())),
            preferred_element_type=F32)

    for copy in loads:
        copy.wait()

    @pl.loop(0, cell_count // 512, unroll=2)
    def _(i):
        turn(field_ref, pl.multiple_of(i * 512, 512), pl.multiple_of(reach + i * 512, 512))

    pad = w_in_full.shape[0]
    w_in_full[pl.ds(pad - 32, 32), :] = jnp.zeros((32, width), BF16)
    w_in_full[pl.ds(0, channels), :] = w_in_ref[...]

    @pl.when(wraps)
    def _():
        pl.semaphore_wait(ready_sem, 1)
        to_far()

    w_in_leave = pltpu.make_async_copy(w_in_full, w_in_out, leave_sem.at[groups + 1])
    w_in_leave.start()
    onward(0)
    across(0, 0, 1)

    field_up.wait_recv()
    field_down.wait_recv()

    begin(1)
    spread(1, 0)

    @pl.when(jnp.logical_not(wrapped))
    def _():
        across(0, 2)

    @pl.loop(0, reach // 512)
    def _(i):
        turn(low_ref, pl.multiple_of(i * 512, 512), pl.multiple_of(i * 512, 512))
        turn(high_ref, pl.multiple_of(i * 512, 512),
             pl.multiple_of(reach + cell_count + i * 512, 512))

    def gather(begin_at, end_at):
        @pl.loop(begin_at, end_at)
        def _(b):
            base = pl.multiple_of(b * slots, slots)
            for j in range(slots):
                picked_ref[pl.ds(base + j, 1), :] = cells_ref[pl.ds(index_ref[b, j], 1), :]

    gather(0, blocks // 2)
    @pl.when(jnp.logical_not(wrapped))
    def _():
        across(0, 3)

    gather(blocks // 2, blocks)
    per_step = 8

    @pl.loop(0, blocks // per_step)
    def _(i):
        for j in range(per_step):
            b = i * per_step + j
            rows_b = picked_ref[pl.ds(pl.multiple_of(b * slots, slots), slots), :].astype(BF16)
            enc_ref[pl.ds(pl.multiple_of(b * per_block, per_block), per_block), :] = jnp.dot(
                weight_ref[b], rows_b, preferred_element_type=F32).astype(BF16)

    enc_far = remote(enc_ref.at[pl.ds(pl.multiple_of(core * margin, margin), margin), :],
                     enc_ref.at[pl.ds(nodes, margin), :], enc_send.at[0], enc_recv.at[0], far)
    enc_far.start()
    enc_leave = pltpu.make_async_copy(enc_ref.at[pl.ds(0, nodes), :], enc_out, leave_sem.at[0])
    enc_leave.start()

    def embed(start, target):
        embedded = jnp.dot(enc_ref[pl.ds(start, 128), :], w_in_full[...], preferred_element_type=F32)
        average = jnp.mean(embedded, axis=1, keepdims=True)
        centered = embedded - average
        spread_of = jnp.mean(centered * centered, axis=1, keepdims=True)
        normed_ref[pl.ds(target, 128), :] = (
            centered * lax.rsqrt(spread_of + 1e-05) * gain_ref[...]).astype(BF16)

    @pl.when(wrapped)
    def _():
        across(0, 2, 3)

    begin(groups)
    spread(groups, 0)
    own = pl.multiple_of(margin + core * nodes, margin)
    theirs = pl.multiple_of(margin + other * nodes, margin)
    edge = pl.multiple_of(core * (window + nodes - margin), margin)
    their_edge = pl.multiple_of(other * (window + nodes - margin), margin)

    def share(i, start):
        ref = normed_ref.at[pl.ds(start, margin), :]
        return remote(ref, ref, nm_send.at[i], nm_recv.at[i], partner)

    for h in range(2):
        @pl.loop(0, 2, unroll=2)
        def _(i):
            embed(pl.multiple_of(h * margin + i * 128, 128), pl.multiple_of(own + h * margin + i * 128, 128))
        share(h, own + h * margin).start()

    same_head = (lax.broadcasted_iota(jnp.int32, (gw, gw), 0) // head_size
                 == lax.broadcasted_iota(jnp.int32, (gw, gw), 1) // head_size).astype(BF16)

    def unit_heads(block, scale):
        squares = block * block
        total = jnp.dot(squares.astype(BF16), same_head, preferred_element_type=F32)
        return (block * lax.rsqrt(total * (1.0 / head_size) + 1e-06)).astype(BF16) * scale

    scale = jnp.asarray(head_size ** -0.5, BF16)
    one = jnp.asarray(1.0, BF16)

    def store_part(g, kind, start, size, part):
        span = pl.ds(start, size)
        if kind == 0:
            q_ref[g, pl.ds(pl.multiple_of(start - margin, margin), size), :] = unit_heads(part, scale)
        elif kind == 1:
            k_ref[g, :, span] = unit_heads(part, one).T
        else:
            v_ref[g, span, :] = part.astype(BF16)

    def rows_of(g, *pieces):
        held = None
        for kind, start, size in pieces:
            part = jnp.dot(normed_ref[pl.ds(start, size), :], qkv_ref[g, :, pl.ds(kind * gw, gw)],
                           preferred_element_type=F32)
            if held is not None:
                store_part(g, *held)
            held = (kind, start, size, part)
        store_part(g, *held)

    def all_of(start, size):
        return [(1, start, size), (0, start, size), (2, start, size)]

    def keys_at(start):
        return [(1, start, margin), (2, start, margin)]

    last(0)

    rows_of(0, *all_of(own, nodes))

    onward(1)
    share(0, theirs).wait_recv()
    share(1, theirs).wait_recv()

    rows_of(0, *all_of(theirs, nodes))
    across(1, 0, 1)
    enc_far.wait_recv()

    @pl.loop(0, 2, unroll=2)
    def _(i):
        embed(pl.multiple_of(nodes + i * 128, 128), pl.multiple_of(edge + i * 128, 128))

    share(2, edge).start()
    rows_of(0, *keys_at(edge))
    share(2, their_edge).wait_recv()
    rows_of(0, *keys_at(their_edge))

    swap = remote(out_ref.at[:, core], out_ref.at[:, core], sw_send.at[0], sw_recv.at[0], partner)

    def attend(g, side, store):
        base = pl.multiple_of(side * nodes, nodes)

        head_of = lax.broadcasted_iota(jnp.int32, (128, gw), 1) // head_size

        def scores_of(i):
            queries = q_ref[g, pl.ds(pl.multiple_of(base + i * 128, 128), 128), :]
            stacked = jnp.concatenate(
                [jnp.where(head_of == h, queries, jnp.zeros_like(queries))
                 for h in range(GROUP_HEADS)], axis=0)
            return jnp.dot(stacked, k_ref[g, :, pl.ds(base, window)], preferred_element_type=F32)

        steps = nodes // 128
        scores = scores_of(0)
        for i in range(steps):
            later = scores_of(i + 1) if i + 1 < steps else None
            weights = jnp.exp(scores)
            total = jnp.sum(weights, axis=1, keepdims=True)
            out = jnp.dot(weights.astype(BF16), v_ref[g, pl.ds(base, window), :],
                          preferred_element_type=F32)
            out = out * (1.0 / total)
            mixed = out[:128]
            for h in range(1, GROUP_HEADS):
                mixed = jnp.where(head_of == h, out[h * 128:(h + 1) * 128], mixed)
            store(pl.ds(i * 128, 128), mixed.astype(BF16))
            scores = later

    def columns(g):
        return att_out.at[:, pl.ds(pl.multiple_of((core * groups + g) * gw, gw), gw)]

    def leave(g):
        return pltpu.make_async_copy(att_ref.at[g], columns(g), leave_sem.at[1 + g])

    def give(g):
        return remote(stage_ref.at[g], columns(g), st_send.at[g], st_recv.at[g], partner)

    for g in range(groups):
        def to_stage(span, value):
            stage_ref[g, span, :] = value

        def to_own(span, value):
            att_ref[g, span, :] = value

        if g == 0:
            onward(groups)
            across(1, 2)
        attend(g, other, to_stage)
        give(g).start()
        if g == 0:
            across(1, 3)
            across(groups, 0)
        else:
            last(groups)
            swap.start()
        attend(g, core, to_own)
        leave(g).start()
        if g == 0:
            across(groups, 1, 2)
            last(1)

            @pl.loop(0, 2)
            def _(i):
                start = pl.multiple_of(margin + i * nodes, margin)
                rows_of(1, *keys_at(pl.multiple_of(i * (window + nodes - margin), margin)), *all_of(start, nodes))

            across(groups, 3)

    swap.wait_recv()
    for g in range(groups):
        give(g).wait_recv()
        leave(g).wait()
    enc_leave.wait()
    w_in_leave.wait()
    for copy in (field_up, field_down, enc_far, swap):
        copy.wait_send()
    for i in range(3):
        share(i, own).wait_send()
    for g in range(groups):
        give(g).wait_send()
    for c in range(groups + 1):
        drain(c)


def project(enc_ref, w_in_ref, att_ref, w_out_ref, latent_ref, update_ref):
    step = latent_ref.shape[0]
    span = pl.ds(pl.multiple_of(pl.program_id(0) * step, step), step)
    latent_ref[...] = jnp.dot(enc_ref[span, :], w_in_ref[...],
                              preferred_element_type=F32).astype(BF16)
    update_ref[...] = jnp.dot(att_ref[span, :], w_out_ref[...],
                              preferred_element_type=F32).astype(BF16)


def shards(n, fields, cell_index, interp_weight, w_in, ln_gain, w_qkv, w_out):
    width = w_out.shape[1]
    blocks, per_block, slots = interp_weight.shape
    nodes = blocks * per_block
    channels, cells = fields.shape[1:]
    reach = cells // 4
    gw = width // HEADS * GROUP_HEADS
    groups = width // gw // 2
    half = w_out.shape[0] // 2
    hbm = pl.BlockSpec(memory_space=pl.ANY)
    free = pl.BlockSpec(memory_space=pl.ANY)
    dma = pltpu.SemaphoreType.DMA
    attended, w_out_full, encoded, w_in_full = pl.pallas_call(
        kernel,
        out_shape=[jax.ShapeDtypeStruct(shape, BF16)
                   for shape in ((nodes, width), (n, 2, half, width), (nodes, 128), (128, width))],
        in_specs=[hbm] * 7,
        out_specs=[free] * 4,
        scratch_shapes=[
            pltpu.SMEM((blocks, slots), jnp.int32),
            pltpu.VMEM((channels, cells), BF16),
            pltpu.VMEM((blocks, per_block, slots), BF16),
            pltpu.VMEM((channels, width), BF16),
            pltpu.VMEM((1, width), F32),
            pltpu.VMEM((channels, reach), BF16),
            pltpu.VMEM((channels, reach), BF16),
            pltpu.VMEM((cells + 2 * reach, 128), F32),
            pltpu.VMEM((blocks * 128, 128), F32),
            pltpu.VMEM((nodes + nodes // 2, 128), BF16),
            pltpu.VMEM((128, width), BF16),
            pltpu.VMEM((3 * nodes, width), BF16),
            pltpu.VMEM((groups, width, 3 * gw), BF16),
            pltpu.VMEM((groups, 2 * nodes, gw), BF16),
            pltpu.VMEM((groups, gw, 3 * nodes), BF16),
            pltpu.VMEM((groups, 3 * nodes, gw), BF16),
            pltpu.VMEM((groups, nodes, gw), BF16),
            pltpu.VMEM((groups, nodes, gw), BF16),
            dma((5,)), dma((3 * groups + 1,)), dma((groups + 2,)),
            dma((2,)), dma((2,)), dma((1,)), dma((1,)),
            dma((3,)), dma((3,)), dma((groups,)), dma((groups,)), dma((1,)), dma((1,)),
            dma((groups + 1, 20)), dma((groups + 1, 20)),
            pltpu.SemaphoreType.REGULAR,
        ],
        compiler_params=pltpu.CompilerParams(
            collective_id=0, has_side_effects=True, vmem_limit_bytes=28 * 2**20),
    )(*(pltpu.with_memory_space_constraint(a, pltpu.HBM) for a in (
        cell_index, fields[0], interp_weight, w_in, ln_gain[None], w_qkv, w_out)))
    w_out_full = w_out_full.reshape(width, width)
    step = nodes // 4

    def by_row(size):
        return pl.BlockSpec((step, size), lambda i: (i, 0))

    vmem = pl.BlockSpec(memory_space=pltpu.VMEM)
    latent, update = pl.pallas_call(
        project,
        grid=(nodes // step,),
        out_shape=[jax.ShapeDtypeStruct((nodes, width), BF16)] * 2,
        in_specs=[vmem] * 4,
        out_specs=[by_row(width), by_row(width)],
        compiler_params=pltpu.CompilerParams(vmem_limit_bytes=24 * 2**20),
    )(encoded, w_in_full, attended, w_out_full)
    return latent[None], update[None]


def solution(mesh):
    placed = (
        P("dp", None, "space"),
        P("space", None),
        P("space", None, None),
        P(),
        P(),
        P("dp", None),
        P("dp", None),
    )
    return jax.shard_map(
        functools.partial(shards, mesh.shape["dp"]),
        mesh=mesh,
        in_specs=placed,
        out_specs=(P("dp", "space", None), P("dp", "space", None)),
        check_vma=False,
    )
```

```python
import functools

import jax
import jax.numpy as jnp
from jax import lax
from jax.experimental import pallas as pl
from jax.experimental.pallas import tpu as pltpu
from jax.sharding import PartitionSpec as P

HEADS = 16
GROUP_HEADS = 4
F32, BF16 = jnp.float32, jnp.bfloat16
MESH = pl.DeviceIdType.MESH
OFFS = (0, -1, 1, 2)


def either(flag, first, second):
    return second if flag else first


def device_at(x, y, z, core):
    return lax.rem(y, 4) * 4 + x, z * 4 + (y // 4) * 2 + core


def kernel(
    index_hbm, field_hbm, weight_hbm, w_in_hbm, gain_hbm, w_qkv_hbm, w_out_hbm,
    att_out, out_ref, enc_out, w_in_out,
    index_ref, field_ref, weight_ref, w_in_ref, gain_ref,
    low_ref, high_ref, cells_ref, picked_ref, enc_ref, w_in_full, normed_ref, qkv_ref,
    q_ref, k_ref, v_ref, result_ref,
    load_sem, local_sem, leave_sem, field_send, field_recv, enc_send, enc_recv,
    nm_send, nm_recv, st_send, st_recv, sw_send, sw_recv, a_send, a_recv, ready_sem,
):
    d, s = lax.axis_index("dp"), lax.axis_index("space")
    x, y_low = lax.rem(d, 4), d // 4
    core, y_high, z = lax.rem(s, 2), lax.rem(s // 2, 2), s // 4
    y = y_high * 4 + y_low
    up, down = lax.rem(s + 1, 32), lax.rem(s + 31, 32)
    other = 1 - core
    partner = (d, s + 1 - 2 * core)
    far = (d, down + core * (up - down))
    wraps, wrapped = s == 0, s == 31

    along_x = [device_at(lax.rem(x + i, 4), y, z, core) for i in (1, 3, 2, 2)]
    along_y = [device_at(x, lax.rem(y + i, 8), z, core) for i in (1, 7, 2, 6)]
    near = along_x[:3] + along_y + [partner]

    barrier = pltpu.get_barrier_semaphore()
    for peer in near:
        pl.semaphore_signal(barrier, inc=1, device_id=peer, device_id_type=MESH)

    @pl.when(jnp.logical_not(wrapped))
    def _():
        pl.semaphore_signal(barrier, inc=1, device_id=far, device_id_type=MESH)

    channels, cell_count = field_ref.shape
    reach = low_ref.shape[1]
    rows = w_qkv_hbm.shape[0]
    width = w_out_hbm.shape[1]
    groups, _, gw3 = qkv_ref.shape
    gw = gw3 // 3
    head_size = gw // GROUP_HEADS
    nodes = result_ref.shape[2]
    margin = nodes // 2
    window = nodes + 2 * margin
    blocks, per_block, slots = weight_ref.shape

    loads = [
        pltpu.make_async_copy(src, dst, load_sem.at[i])
        for i, (src, dst) in enumerate((
            (field_hbm, field_ref), (index_hbm, index_ref), (weight_hbm, weight_ref),
            (w_in_hbm, w_in_ref), (gain_hbm, gain_ref)))]
    local = []
    for g in range(groups):
        for t in range(3):
            local.append(pltpu.make_async_copy(
                w_qkv_hbm.at[:, pl.ds(pl.multiple_of(t * width + core * (width // 2) + g * gw, gw), gw)],
                qkv_ref.at[g, pl.ds(pl.multiple_of(d * rows, rows), rows), pl.ds(t * gw, gw)],
                local_sem.at[len(local)]))
    half = rows // 2
    local.append(pltpu.make_async_copy(
        w_out_hbm.at[pl.ds(pl.multiple_of(core * half, half), half), :], out_ref.at[d, core],
        local_sem.at[len(local)]))
    for copy in local[:3] + loads[:1] + local[3:] + loads[1:]:
        copy.start()

    pl.semaphore_wait(barrier, len(near) + 1 - wraps.astype(jnp.int32))

    @pl.when(wrapped)
    def _():
        pl.semaphore_signal(ready_sem, inc=1, device_id=far, device_id_type=MESH)

    def remote(src, dst, send, recv, device):
        return pltpu.make_async_remote_copy(
            src_ref=src, dst_ref=dst, send_sem=send, recv_sem=recv,
            device_id=device, device_id_type=MESH)

    field_up = remote(field_hbm.at[:, pl.ds(cell_count - reach, reach)], low_ref,
                      field_send.at[0], field_recv.at[0], (d, up))
    field_down = remote(field_hbm.at[:, pl.ds(0, reach)], high_ref,
                        field_send.at[1], field_recv.at[1], (d, down))

    def to_far():
        @pl.when(core == 0)
        def _():
            field_down.start()

        @pl.when(core == 1)
        def _():
            field_up.start()

    @pl.when(core == 0)
    def _():
        field_up.start()

    @pl.when(core == 1)
    def _():
        field_down.start()

    turns = (1, 1, 0)

    def slot(c, i, j):
        place1, place2 = x + turns[c] * (y_low - x), y_low + turns[c] * (x - y_low)
        return (lax.rem(place1 + i + 4, 4) * (1 + 3 * turns[c])
                + lax.rem(place2 + j + 4, 4) * (4 - 3 * turns[c]))

    def piece(c, at, side=None):
        if c < groups:
            lo, size = (0, rows) if side is None else (side * half, half)
            return qkv_ref.at[c, pl.ds(pl.multiple_of(at * rows + lo, size), size), :]
        lo, size = (0, half) if side is None else (side * (half // 2), half // 2)
        return out_ref.at[at, core, pl.ds(lo, size), :]

    sides = (None, None, 0, 1)

    def hop(c, i, at, device):
        ref = piece(c, at, sides[i % 4])
        return remote(ref, ref, a_send.at[c, i], a_recv.at[c, i], device)

    def begin(c):
        for copy in local[3 * c:3 * c + 3] if c < groups else local[-1:]:
            copy.wait()
        for i in range(4):
            hop(c, i, slot(c, 0, 0), either(turns[c], along_x[i], along_y[i])).start()

    def spread(c, j):
        for i in range(2):
            hop(c, 4 + 4 * j + i, slot(c, OFFS[j], 0), either(turns[c], along_y[i], along_x[i])).start()

    def onward(c):
        hop(c, 0, slot(c, -1, 0), partner).wait_recv()
        spread(c, 1)
        hop(c, 1, slot(c, 1, 0), partner).wait_recv()
        spread(c, 2)
        hop(c, 2, slot(c, 2, 0), partner).wait_recv()
        hop(c, 3, slot(c, 2, 0), partner).wait_recv()
        spread(c, 3)

    def across(c, *js):
        for j in js:
            for i in range(2):
                at = slot(c, OFFS[j], 2 * i - 1)
                hop(c, 4 + 4 * j + i, at, partner).wait_recv()
                hop(c, 6 + 4 * j + i, at, either(turns[c], along_y[i], along_x[i])).start()

    def last(c):
        for j in range(4):
            for i in range(2):
                hop(c, 6 + 4 * j + i, slot(c, OFFS[j], 2), partner).wait_recv()

    def drain(c):
        for i in range(20):
            hop(c, i, slot(c, 0, 0), partner).wait_send()

    @pl.when(wrapped)
    def _():
        to_far()

    begin(0)

    @pl.when(jnp.logical_not(wraps | wrapped))
    def _():
        to_far()

    spread(0, 0)

    unit = (lax.broadcasted_iota(jnp.int32, (channels, 128), 0)
            == lax.broadcasted_iota(jnp.int32, (channels, 128), 1)).astype(BF16)

    def turn(source, start, target):
        cells_ref[pl.ds(target, 512), :] = lax.dot_general(
            source[:, pl.ds(start, 512)], unit, (((0,), (0,)), ((), ())),
            preferred_element_type=F32)

    for copy in loads:
        copy.wait()

    @pl.loop(0, cell_count // 512, unroll=2)
    def _(i):
        turn(field_ref, pl.multiple_of(i * 512, 512), pl.multiple_of(reach + i * 512, 512))

    pad = w_in_full.shape[0]
    w_in_full[pl.ds(pad - 32, 32), :] = jnp.zeros((32, width), BF16)
    w_in_full[pl.ds(0, channels), :] = w_in_ref[...]

    @pl.when(wraps)
    def _():
        pl.semaphore_wait(ready_sem, 1)
        to_far()

    w_in_leave = pltpu.make_async_copy(w_in_full, w_in_out, leave_sem.at[groups + 1])
    w_in_leave.start()
    onward(0)
    def begin_next():
        begin(1)
        spread(1, 0)

    pl.when(s < 4)(begin_next)
    across(0, 0, 1)

    field_up.wait_recv()
    field_down.wait_recv()

    pl.when(s >= 4)(begin_next)

    @pl.when(jnp.logical_not(wrapped))
    def _():
        across(0, 2)

    @pl.loop(0, reach // 512)
    def _(i):
        turn(low_ref, pl.multiple_of(i * 512, 512), pl.multiple_of(i * 512, 512))
        turn(high_ref, pl.multiple_of(i * 512, 512),
             pl.multiple_of(reach + cell_count + i * 512, 512))

    def gather(begin_at, end_at):
        @pl.loop(begin_at, end_at)
        def _(b):
            base = pl.multiple_of(b * slots, slots)
            for j in range(slots):
                picked_ref[pl.ds(base + j, 1), :] = cells_ref[pl.ds(index_ref[b, j], 1), :]

    gather(0, blocks // 2)
    @pl.when(jnp.logical_not(wrapped))
    def _():
        across(0, 3)

    gather(blocks // 2, blocks)
    per_step = 8

    @pl.loop(0, blocks // per_step)
    def _(i):
        for j in range(per_step):
            b = i * per_step + j
            rows_b = picked_ref[pl.ds(pl.multiple_of(b * slots, slots), slots), :].astype(BF16)
            enc_ref[pl.ds(pl.multiple_of(b * per_block, per_block), per_block), :] = jnp.dot(
                weight_ref[b], rows_b, preferred_element_type=F32).astype(BF16)

    enc_far = remote(enc_ref.at[pl.ds(pl.multiple_of(core * margin, margin), margin), :],
                     enc_ref.at[pl.ds(nodes, margin), :], enc_send.at[0], enc_recv.at[0], far)
    enc_far.start()
    enc_leave = pltpu.make_async_copy(enc_ref.at[pl.ds(0, nodes), :], enc_out, leave_sem.at[0])
    enc_leave.start()

    def embed(start, target):
        embedded = jnp.dot(enc_ref[pl.ds(start, 128), :], w_in_full[...], preferred_element_type=F32)
        average = jnp.mean(embedded, axis=1, keepdims=True)
        centered = embedded - average
        spread_of = jnp.mean(centered * centered, axis=1, keepdims=True)
        normed_ref[pl.ds(target, 128), :] = (
            centered * lax.rsqrt(spread_of + 1e-05) * gain_ref[...]).astype(BF16)

    @pl.when(wrapped)
    def _():
        across(0, 2, 3)

    begin(groups)
    spread(groups, 0)
    own = pl.multiple_of(margin + core * nodes, margin)
    theirs = pl.multiple_of(margin + other * nodes, margin)
    edge = pl.multiple_of(core * (window + nodes - margin), margin)
    their_edge = pl.multiple_of(other * (window + nodes - margin), margin)

    def share(i, start):
        ref = normed_ref.at[pl.ds(start, margin), :]
        return remote(ref, ref, nm_send.at[i], nm_recv.at[i], partner)

    for h in range(2):
        @pl.loop(0, 2, unroll=2)
        def _(i):
            embed(pl.multiple_of(h * margin + i * 128, 128), pl.multiple_of(own + h * margin + i * 128, 128))
        share(h, own + h * margin).start()

    same_head = (lax.broadcasted_iota(jnp.int32, (gw, gw), 0) // head_size
                 == lax.broadcasted_iota(jnp.int32, (gw, gw), 1) // head_size).astype(BF16)

    def unit_heads(block, scale):
        squares = block * block
        total = jnp.dot(squares.astype(BF16), same_head, preferred_element_type=F32)
        return (block * lax.rsqrt(total * (1.0 / head_size) + 1e-06)).astype(BF16) * scale

    scale = jnp.asarray(head_size ** -0.5, BF16)
    one = jnp.asarray(1.0, BF16)

    def store_part(g, kind, start, size, part):
        span = pl.ds(start, size)
        if kind == 0:
            q_ref[g, pl.ds(pl.multiple_of(start - margin, margin), size), :] = unit_heads(part, scale)
        elif kind == 1:
            k_ref[g, :, span] = unit_heads(part, one).T
        else:
            v_ref[g, span, :] = part.astype(BF16)

    def rows_of(g, *pieces):
        held = None
        for kind, start, size in pieces:
            part = jnp.dot(normed_ref[pl.ds(start, size), :], qkv_ref[g, :, pl.ds(kind * gw, gw)],
                           preferred_element_type=F32)
            if held is not None:
                store_part(g, *held)
            held = (kind, start, size, part)
        store_part(g, *held)

    def all_of(start, size):
        return [(1, start, size), (0, start, size), (2, start, size)]

    def keys_at(start):
        return [(1, start, margin), (2, start, margin)]

    last(0)

    rows_of(0, *all_of(own, nodes))

    onward(1)
    share(0, theirs).wait_recv()
    share(1, theirs).wait_recv()

    rows_of(0, *all_of(theirs, nodes))
    across(1, 0)

    @pl.when(s < 2)
    def _():
        across(1, 1)

    def own_edge():
        enc_far.wait_recv()

        @pl.loop(0, 2, unroll=2)
        def _(i):
            embed(pl.multiple_of(nodes + i * 128, 128), pl.multiple_of(edge + i * 128, 128))

        share(2, edge).start()
        rows_of(0, *keys_at(edge))

    def other_edge():
        share(2, their_edge).wait_recv()
        rows_of(0, *keys_at(their_edge))

    pl.when(s != 0)(own_edge)
    @pl.when(s >= 2)
    def _():
        across(1, 1)

    pl.when(s != 1)(other_edge)

    swap = remote(out_ref.at[:, core], out_ref.at[:, core], sw_send.at[0], sw_recv.at[0], partner)

    def attend(g, side, store):
        base = pl.multiple_of(side * nodes, nodes)

        head_of = lax.broadcasted_iota(jnp.int32, (128, gw), 1) // head_size

        def scores_of(i):
            queries = q_ref[g, pl.ds(pl.multiple_of(base + i * 128, 128), 128), :]
            stacked = jnp.concatenate(
                [jnp.where(head_of == h, queries, jnp.zeros_like(queries))
                 for h in range(GROUP_HEADS)], axis=0)
            return jnp.dot(stacked, k_ref[g, :, pl.ds(base, window)], preferred_element_type=F32)

        steps = nodes // 128
        scores = scores_of(0)
        for i in range(steps):
            later = scores_of(i + 1) if i + 1 < steps else None
            weights = jnp.exp(scores)
            total = jnp.sum(weights, axis=1, keepdims=True)
            out = jnp.dot(weights.astype(BF16), v_ref[g, pl.ds(base, window), :],
                          preferred_element_type=F32)
            out = out * (1.0 / total)
            mixed = out[:128]
            for h in range(1, GROUP_HEADS):
                mixed = jnp.where(head_of == h, out[h * 128:(h + 1) * 128], mixed)
            store(pl.ds(i * 128, 128), mixed.astype(BF16))
            scores = later

    def columns(g):
        return att_out.at[:, pl.ds(pl.multiple_of((core * groups + g) * gw, gw), gw)]

    def leave(g):
        return pltpu.make_async_copy(result_ref.at[1, g], columns(g), leave_sem.at[1 + g])

    def give(g):
        return remote(result_ref.at[0, g], columns(g), st_send.at[g], st_recv.at[g], partner)

    swapped = (s == 1).astype(jnp.int32)
    for g in range(groups):
        earlier = swapped if g == 0 else 0

        def to_place(place):
            def store(span, value):
                result_ref[place, g, span, :] = value
            return store

        if g == 0:
            onward(groups)
            across(1, 2)
        attend(g, other + earlier * (core - other), to_place(earlier))
        if g == 0:
            across(1, 3)
            across(groups, 0)
            pl.when(s == 0)(own_edge)
            pl.when(s == 1)(other_edge)
        else:
            last(groups)
            swap.start()
            give(g).start()
        attend(g, core + earlier * (other - core), to_place(1 - earlier))
        leave(g).start()
        if g == 0:
            give(g).start()
            across(groups, 1, 2, 3)
            last(1)

            @pl.loop(0, 2)
            def _(i):
                start = pl.multiple_of(margin + i * nodes, margin)
                rows_of(1, *keys_at(pl.multiple_of(i * (window + nodes - margin), margin)), *all_of(start, nodes))

    swap.wait_recv()
    for g in range(groups):
        give(g).wait_recv()
        leave(g).wait()
    enc_leave.wait()
    w_in_leave.wait()
    for copy in (field_up, field_down, enc_far, swap):
        copy.wait_send()
    for i in range(3):
        share(i, own).wait_send()
    for g in range(groups):
        give(g).wait_send()
    for c in range(groups + 1):
        drain(c)


def project(enc_ref, w_in_ref, att_ref, w_out_ref, latent_ref, update_ref):
    step = latent_ref.shape[0]
    span = pl.ds(pl.multiple_of(pl.program_id(0) * step, step), step)
    latent_ref[...] = jnp.dot(enc_ref[span, :], w_in_ref[...],
                              preferred_element_type=F32).astype(BF16)
    update_ref[...] = jnp.dot(att_ref[span, :], w_out_ref[...],
                              preferred_element_type=F32).astype(BF16)


def shards(n, fields, cell_index, interp_weight, w_in, ln_gain, w_qkv, w_out):
    width = w_out.shape[1]
    blocks, per_block, slots = interp_weight.shape
    nodes = blocks * per_block
    channels, cells = fields.shape[1:]
    reach = cells // 4
    gw = width // HEADS * GROUP_HEADS
    groups = width // gw // 2
    half = w_out.shape[0] // 2
    hbm = pl.BlockSpec(memory_space=pl.ANY)
    free = pl.BlockSpec(memory_space=pl.ANY)
    dma = pltpu.SemaphoreType.DMA
    attended, w_out_full, encoded, w_in_full = pl.pallas_call(
        kernel,
        out_shape=[jax.ShapeDtypeStruct(shape, BF16)
                   for shape in ((nodes, width), (n, 2, half, width), (nodes, 128), (128, width))],
        in_specs=[hbm] * 7,
        out_specs=[free] * 4,
        scratch_shapes=[
            pltpu.SMEM((blocks, slots), jnp.int32),
            pltpu.VMEM((channels, cells), BF16),
            pltpu.VMEM((blocks, per_block, slots), BF16),
            pltpu.VMEM((channels, width), BF16),
            pltpu.VMEM((1, width), F32),
            pltpu.VMEM((channels, reach), BF16),
            pltpu.VMEM((channels, reach), BF16),
            pltpu.VMEM((cells + 2 * reach, 128), F32),
            pltpu.VMEM((blocks * 128, 128), F32),
            pltpu.VMEM((nodes + nodes // 2, 128), BF16),
            pltpu.VMEM((128, width), BF16),
            pltpu.VMEM((3 * nodes, width), BF16),
            pltpu.VMEM((groups, width, 3 * gw), BF16),
            pltpu.VMEM((groups, 2 * nodes, gw), BF16),
            pltpu.VMEM((groups, gw, 3 * nodes), BF16),
            pltpu.VMEM((groups, 3 * nodes, gw), BF16),
            pltpu.VMEM((2, groups, nodes, gw), BF16),
            dma((5,)), dma((3 * groups + 1,)), dma((groups + 2,)),
            dma((2,)), dma((2,)), dma((1,)), dma((1,)),
            dma((3,)), dma((3,)), dma((groups,)), dma((groups,)), dma((1,)), dma((1,)),
            dma((groups + 1, 20)), dma((groups + 1, 20)),
            pltpu.SemaphoreType.REGULAR,
        ],
        compiler_params=pltpu.CompilerParams(
            collective_id=0, has_side_effects=True, vmem_limit_bytes=28 * 2**20),
    )(*(pltpu.with_memory_space_constraint(a, pltpu.HBM) for a in (
        cell_index, fields[0], interp_weight, w_in, ln_gain[None], w_qkv, w_out)))
    w_out_full = w_out_full.reshape(width, width)
    step = nodes // 4

    def by_row(size):
        return pl.BlockSpec((step, size), lambda i: (i, 0))

    vmem = pl.BlockSpec(memory_space=pltpu.VMEM)
    latent, update = pl.pallas_call(
        project,
        grid=(nodes // step,),
        out_shape=[jax.ShapeDtypeStruct((nodes, width), BF16)] * 2,
        in_specs=[vmem] * 4,
        out_specs=[by_row(width), by_row(width)],
        compiler_params=pltpu.CompilerParams(vmem_limit_bytes=24 * 2**20),
    )(encoded, w_in_full, attended, w_out_full)
    return latent[None], update[None]


def solution(mesh):
    placed = (
        P("dp", None, "space"),
        P("space", None),
        P("space", None, None),
        P(),
        P(),
        P("dp", None),
        P("dp", None),
    )
    return jax.shard_map(
        functools.partial(shards, mesh.shape["dp"]),
        mesh=mesh,
        in_specs=placed,
        out_specs=(P("dp", "space", None), P("dp", "space", None)),
        check_vma=False,
    )
```
